32 devices in a mesh: gx: 8 (over y, x, core), gy: 4 (over z).
Axes of the slice: x: 2, y: 2, z: 4, core: 2. Of those that a mesh axis runs over, the one named last changes fastest.
Arguments:
- ocean_heat_field: float32 [8, 192, 128, 128], P('gy', 'gx'), may hold values from -6 to 6
- patch_zone: int32 [192], replicated, may hold values from 0 to 31, as said below
- patch_position: int32 [192], replicated, may hold values from 0 to 11, as said below
- quarter_spins: int32 [192], replicated, may hold values from 0 to 3
- zone_patch_tally: int32 [32], P(('gx', 'gy')), may hold values from 0 to 12, as said below
Outputs:
- regional: float32 [8, 32, 12, 128, 128], P(None, ('gx', 'gy'))
The draws below stay inside these ranges and needn't reach their ends.
Inputs may be any that keep to these rules, and one draw needn't show every extreme that they name: In each aligned group of 24 blocks no more than 6 go to regions of one column patch_zone // 4, and each group has a column with exactly 6. A region receives at most 12 blocks and some region receives exactly 12. `patch_position`: the blocks of one region have distinct slots 0 to zone_patch_tally of that region minus 1, in increasing block order. zone_patch_tally[r] is the number of blocks j with patch_zone[j] = r.
All inputs are finite; a program needn't handle non-finite values.
Results may differ from the reference program's by a relative error of at most 0.00002.
Values sent between devices are 32-bit elements; how exact they have to be, the bound alone decides.
No kernel may reach another device: no remote copies, remote signals or barrier semaphores. Data moves between devices by JAX's collectives and lax.ppermute only.
A program may use at most 128 MiB of HBM per device.

```python
import jax
import jax.numpy as jnp

PATCH_SIDE = 128
BLK_DEV = 24
INPUT_PATCHES = 192
EPOCH_TOTAL = 8
REGIONS = 32
MOST = 6
CAP = 12


def rank_within(labels, label_count):
    onehot = (labels[:, None] == jnp.arange(label_count, dtype=jnp.int32)[None, :]).astype(jnp.int32)
    running = jnp.cumsum(onehot, axis=0) - onehot
    return jnp.sum(running * onehot, axis=1).astype(jnp.int32)


def routing(key):
    column_count = INPUT_PATCHES // BLK_DEV
    row_count = REGIONS // column_count
    column_slots = column_count * MOST
    group_key = jax.random.fold_in(key, 101)
    order_key = jax.random.fold_in(key, 202)

    def group_columns(subkey):
        pick_key, score_key, shuffle_key = jax.random.split(subkey, 3)
        chosen = jax.random.randint(pick_key, (), 0, column_count, dtype=jnp.int32)
        slot_ids = jnp.arange(column_slots, dtype=jnp.int32)
        scores = jax.random.permutation(score_key, column_slots).astype(jnp.int32)
        scores = jnp.where(slot_ids // MOST == chosen, slot_ids % MOST - MOST, scores)
        ranked = jnp.argsort(scores, stable=True).astype(jnp.int32)
        return jax.random.permutation(shuffle_key, ranked[:BLK_DEV] // MOST)
    columns = jax.vmap(group_columns)(jax.random.split(group_key, column_count)).reshape(-1)

    def column_order(subkey):
        pick_key, score_key = jax.random.split(subkey)
        chosen = jax.random.randint(pick_key, (), 0, row_count, dtype=jnp.int32)
        slot_ids = jnp.arange(column_slots, dtype=jnp.int32)
        scores = jax.random.permutation(score_key, column_slots).astype(jnp.int32)
        scores = jnp.where(slot_ids // CAP == chosen, slot_ids % CAP - CAP, scores)
        return jnp.argsort(scores, stable=True).astype(jnp.int32)
    orders = jax.vmap(column_order)(jax.random.split(order_key, column_count))
    within = rank_within(columns, column_count)
    rows = orders[columns, within] // CAP
    regions = (columns * row_count + rows).astype(jnp.int32)
    slots = rank_within(regions, REGIONS)
    counts = jnp.sum((regions[:, None] == jnp.arange(REGIONS, dtype=jnp.int32)[None, :]).astype(jnp.int32), axis=0)
    return (regions, slots, counts.astype(jnp.int32))


def draw_patch_zone(key, part):
    return routing(key)[0]


def draw_patch_position(key, part):
    return routing(key)[1]


def draw_zone_patch_tally(key, part):
    return routing(key)[2]


def plant(array, key, smallest, largest):
    shape = array.shape
    index_at = [jax.random.randint(jax.random.fold_in(key, axis), (), 0, shape[axis]) for axis in range(len(shape))]
    array = array.at[tuple(index_at)].set(smallest)
    longest = shape.index(max(shape))
    index_at[longest] = (index_at[longest] + 1) % shape[longest]
    return array.at[tuple(index_at)].set(largest)


def level_of(rng, extent, pieces, low, high):
    def one(axis_at, blocks):
        heights = jax.random.uniform(jax.random.fold_in(jax.random.fold_in(rng, 6), axis_at), (blocks,), jnp.float32, low / len(pieces), high / len(pieces))
        return jnp.repeat(jnp.exp(heights), extent[axis_at] // blocks).reshape((-1,) + (1,) * (len(extent) - axis_at - 1))

    loudness = one(*pieces[0])
    for cut in pieces[1:]:
        loudness = loudness * one(*cut)
    return loudness


def noise(rng, dims, deviation, limit, cuts=(), kind=jnp.bfloat16):
    result = jax.random.normal(rng, dims, jnp.float32) * deviation
    if len(cuts) > 0:
        result = level_of(rng, dims, cuts, -0.22, 0.18) * result
    return jnp.clip(result, min=-limit, max=limit).astype(kind)


def setup_inputs(seed: int = 0) -> dict:
    streams_of = jax.random.split(jax.random.key(seed), 6)
    return {
        "ocean_heat_field": noise(streams_of[0], (EPOCH_TOTAL, INPUT_PATCHES, PATCH_SIDE, PATCH_SIDE), 1.0, 6.0, ((0, 4), (1, 8)), jnp.float32),
        "patch_zone": draw_patch_zone(jax.random.fold_in(streams_of[5], 71), 0),
        "patch_position": draw_patch_position(jax.random.fold_in(streams_of[5], 71), 0),
        "quarter_spins": plant(jax.random.randint(streams_of[3], (INPUT_PATCHES,), 0, 4), jax.random.fold_in(streams_of[3], 1), 0, 3).astype(jnp.int32),
        "zone_patch_tally": draw_zone_patch_tally(jax.random.fold_in(streams_of[5], 71), 0),
    }


def spin_patches(incoming_patches, turn_codes):
    first_turn = jnp.rot90(incoming_patches, 1, axes=(2, 3))
    half_turn = jnp.rot90(incoming_patches, 2, axes=(2, 3))
    last_turn = jnp.rot90(incoming_patches, 3, axes=(2, 3))
    shaped = turn_codes[None, :, None, None]
    return jnp.where(shaped == 0, incoming_patches, jnp.where(shaped == 1, first_turn, jnp.where(shaped == 2, half_turn, last_turn)))


def reference(ocean_heat_field, patch_zone, patch_position, quarter_spins, zone_patch_tally):
    spun_patches = spin_patches(ocean_heat_field, quarter_spins)
    centered = spun_patches - jnp.mean(spun_patches, axis=0, keepdims=True)
    arranged = jnp.zeros((EPOCH_TOTAL, REGIONS, CAP, PATCH_SIDE, PATCH_SIDE), jnp.float32)
    arranged = arranged.at[:, patch_zone, patch_position].set(centered)
    in_use = jnp.arange(CAP, dtype=jnp.int32)[None, :] < zone_patch_tally[:, None]
    return jnp.where(in_use[None, :, :, None, None], arranged, jnp.float32(0.0))
```

```python
import functools

import jax
import jax.numpy as jnp
from jax import lax
from jax.experimental import pallas as pl
from jax.experimental.pallas import tpu as pltpu
from jax.sharding import PartitionSpec as P

CHUNKS = 4

SMEM = pl.BlockSpec(memory_space=pltpu.SMEM)
VMEM = pl.BlockSpec(memory_space=pltpu.VMEM)


def select_dot(a, b, contract_b):
    return lax.dot_general(
        a,
        b,
        (((1,), (contract_b,)), ((), ())),
        precision=lax.Precision.HIGHEST,
        preferred_element_type=jnp.float32,
    )


def pack_kernel(first_row, rows, places, turns, x_ref, out_ref):
    steps, blocks, side, _ = x_ref.shape
    row = lax.broadcasted_iota(jnp.int32, (rows, side), 0) + first_row
    lane = lax.broadcasted_iota(jnp.int32, (rows, side), 1)
    keep = (lane == row).astype(jnp.float32)
    flip = (lane == side - 1 - row).astype(jnp.float32)
    whole_row = lax.broadcasted_iota(jnp.int32, (side, side), 0)
    whole_lane = lax.broadcasted_iota(jnp.int32, (side, side), 1)
    mirror = (whole_lane == side - 1 - whole_row).astype(jnp.float32)

    def one(j, carry):
        place = places[j]
        turn = turns[j]

        @pl.when(turn == 0)
        def _():
            for t in range(steps):
                out_ref[place, t] = x_ref[t, j, pl.ds(first_row, rows), :]

        @pl.when(turn == 1)
        def _():
            for t in range(steps):
                out_ref[place, t] = select_dot(flip, x_ref[t, j], 1)

        @pl.when(turn == 2)
        def _():
            for t in range(steps):
                out_ref[place, t] = select_dot(select_dot(flip, x_ref[t, j], 0), mirror, 0)

        @pl.when(turn == 3)
        def _():
            for t in range(steps):
                out_ref[place, t] = select_dot(select_dot(keep, x_ref[t, j], 1), mirror, 0)

        return carry

    lax.fori_loop(0, blocks, one, 0)


def pick_kernel(source, arrived_ref, out_ref):
    def one(s, carry):
        at = source[s]

        @pl.when(at >= 0)
        def _():
            out_ref[s] = arrived_ref[at]

        return carry

    lax.fori_loop(0, out_ref.shape[0], one, 0)


def center_kernel(tally, *refs):
    z_ref, out_ref = refs[0], refs[-1]
    groups, slots, steps, rows, side = z_ref.shape
    first_slot = pl.program_id(0) * slots
    for s in range(slots):
        used = first_slot + s < tally[0]

        @pl.when(used)
        def _():
            values = z_ref[:, s].reshape(groups * steps, rows, side)
            mean = jnp.sum(values, axis=0, keepdims=True) * (1.0 / (groups * steps))
            out_ref[:, 0, s] = values - mean

        @pl.when(jnp.logical_not(used))
        def _():
            out_ref[:, 0, s] = jnp.zeros((groups * steps, rows, side), jnp.float32)


def on_device(ocean_heat_field, patch_zone, patch_position, quarter_spins, zone_patch_tally):
    steps, patches, side, _ = ocean_heat_field.shape
    columns = lax.axis_size("gx")
    row_count = lax.axis_size("gy")
    per_peer = 2 * patches // columns
    capacity = 2 * patches // row_count
    rows = side // CHUNKS
    me = lax.axis_index("gx")

    column = (patch_zone // row_count).reshape(columns, patches)
    same = column[:, :, None] == column[:, None, :]
    earlier = jnp.arange(patches)[None, None, :] < jnp.arange(patches)[None, :, None]
    rank = jnp.sum((same & earlier).astype(jnp.int32), axis=2)
    my_column = lax.dynamic_index_in_dim(column, me, 0, keepdims=False)
    my_rank = lax.dynamic_index_in_dim(rank, me, 0, keepdims=False)
    places = my_column * per_peer + my_rank
    turns = lax.dynamic_slice_in_dim(quarter_spins, me * patches, patches)
    arrival = (jnp.arange(columns, dtype=jnp.int32)[:, None] * per_peer + rank).reshape(-1)
    first_target = me * row_count * capacity
    targets = first_target + jnp.arange(row_count * capacity, dtype=jnp.int32)
    flat_dest = patch_zone * capacity + patch_position
    matched = flat_dest[None, :] == targets[:, None]
    source = jnp.sum(jnp.where(matched, arrival[None, :] + 1, 0), axis=1) - 1

    per_step = capacity // 3
    out_shape = jax.ShapeDtypeStruct(
        (steps * row_count, 1, capacity, side, side), jnp.float32
    )
    regional = None
    for k in range(CHUNKS):
        packed = pl.pallas_call(
            functools.partial(pack_kernel, k * rows, rows),
            out_shape=jax.ShapeDtypeStruct(
                (columns * per_peer, steps, rows, side), jnp.float32
            ),
            in_specs=[SMEM, SMEM, VMEM],
            out_specs=VMEM,
            name=f"pack{k}",
        )(places, turns, ocean_heat_field)
        arrived = lax.all_to_all(packed, "gx", split_axis=0, concat_axis=0, tiled=True)
        picked = pl.pallas_call(
            pick_kernel,
            out_shape=jax.ShapeDtypeStruct(
                (row_count * capacity, steps, rows, side), jnp.float32
            ),
            in_specs=[SMEM, VMEM],
            out_specs=VMEM,
            name="pick",
        )(source, arrived)
        timed = lax.all_to_all(picked, "gy", split_axis=0, concat_axis=0, tiled=True)
        timed = timed.reshape(row_count, capacity, steps, rows, side)
        operands = (zone_patch_tally, timed) + (() if k == 0 else (regional,))
        regional = pl.pallas_call(
            center_kernel,
            grid=(capacity // per_step,),
            out_shape=out_shape,
            in_specs=[
                SMEM,
                pl.BlockSpec((row_count, per_step, steps, rows, side), lambda i: (0, i, 0, 0, 0)),
            ]
            + ([] if k == 0 else [pl.BlockSpec(memory_space=pl.ANY)]),
            out_specs=pl.BlockSpec(
                (steps * row_count, 1, per_step, rows, side),
                functools.partial(lambda k, i: (0, 0, i, k, 0), k),
            ),
            input_output_aliases={} if k == 0 else {2: 0},
            name=f"center{k}",
        )(*operands)
    return regional


def solution(mesh):
    placed = (P("gy", "gx", None, None), P(), P(), P(), P(("gx", "gy")))
    return jax.shard_map(
        on_device,
        mesh=mesh,
        in_specs=placed,
        out_specs=P(None, ("gx", "gy"), None, None, None),
        check_vma=False,
    )
```

```python
import functools

import jax
import jax.numpy as jnp
from jax import lax
from jax.experimental import pallas as pl
from jax.experimental.pallas import tpu as pltpu
from jax.sharding import PartitionSpec as P

CHUNKS = 4


SMEM = pl.BlockSpec(memory_space=pltpu.SMEM)
VMEM = pl.BlockSpec(memory_space=pltpu.VMEM)


def dot(a, b, contract_b):
    return lax.dot_general(
        a, b, (((1,), (contract_b,)), ((), ())), preferred_element_type=jnp.float32
    )


def pack_kernel(first_row, rows, peers, ranks, turns, x_ref, *out_refs):
    steps, blocks, side, _ = x_ref.shape
    row = lax.broadcasted_iota(jnp.int32, (rows, side), 0) + first_row
    lane = lax.broadcasted_iota(jnp.int32, (rows, side), 1)
    whole_row = lax.broadcasted_iota(jnp.int32, (side, side), 0)
    whole_lane = lax.broadcasted_iota(jnp.int32, (side, side), 1)

    def turned(j):
        turn = turns[j]
        flip_rows = jnp.logical_or(turn == 1, turn == 2)
        flip_lanes = turn >= 2
        left = (lane == jnp.where(flip_rows, side - 1 - row, row)).astype(jnp.bfloat16)
        right = (
            whole_lane == jnp.where(flip_lanes, side - 1 - whole_row, whole_row)
        ).astype(jnp.bfloat16)
        odd = turn % 2 == 1
        result = []
        for t in range(steps):
            x = x_ref[t, j]
            total = None
            for _ in range(3):
                part = x.astype(jnp.bfloat16)
                x = x - part.astype(jnp.float32)
                moved = jnp.where(odd, dot(left, part, 1), dot(left, part, 0))
                moved = dot(moved.astype(jnp.bfloat16), right, 0)
                total = moved if total is None else total + moved
            result.append(total)
        return result

    unroll = 4

    def some(i, carry):
        for u in range(unroll):
            j = i * unroll + u
            result = turned(j)
            for d, out_ref in enumerate(out_refs):

                @pl.when(peers[j] == d)
                def _():
                    for t in range(steps):
                        out_ref[ranks[j], t] = result[t]

        return carry

    lax.fori_loop(0, blocks // unroll, some, 0)


def pick_kernel(target, *refs):
    arrived_refs, out_ref = refs[:-1], refs[-1]
    per_peer = arrived_refs[0].shape[0]
    for d, arrived_ref in enumerate(arrived_refs):
        for i in range(per_peer):
            to = target[d * per_peer + i]

            @pl.when(to >= 0)
            def _():
                out_ref[to] = arrived_ref[i]


def center_kernel(tally, *refs):
    z_ref, out_ref = refs[0], refs[-1]
    groups, slots, steps, rows, side = z_ref.shape
    first_slot = pl.program_id(0) * slots
    for s in range(slots):
        used = first_slot + s < tally[0]

        @pl.when(used)
        def _():
            values = z_ref[:, s].reshape(groups * steps, rows, side)
            mean = jnp.sum(values, axis=0, keepdims=True) * (1.0 / (groups * steps))
            out_ref[:, 0, s] = values - mean

        @pl.when(jnp.logical_not(used))
        def _():
            out_ref[:, 0, s] = jnp.zeros((groups * steps, rows, side), jnp.float32)


def on_device(ocean_heat_field, patch_zone, patch_position, quarter_spins, zone_patch_tally):
    steps, patches, side, _ = ocean_heat_field.shape
    columns = lax.axis_size("gx")
    row_count = lax.axis_size("gy")
    per_peer = 2 * patches // columns
    capacity = 2 * patches // row_count
    rows = side // CHUNKS
    me = lax.axis_index("gx")

    column = (patch_zone // row_count).reshape(columns, patches)
    same = column[:, :, None] == column[:, None, :]
    earlier = jnp.arange(patches)[None, None, :] < jnp.arange(patches)[None, :, None]
    rank = jnp.sum((same & earlier).astype(jnp.int32), axis=2)
    my_column = lax.dynamic_index_in_dim(column, me, 0, keepdims=False)
    my_rank = lax.dynamic_index_in_dim(rank, me, 0, keepdims=False)
    peers = jnp.bitwise_xor(my_column, me)
    turns = lax.dynamic_slice_in_dim(quarter_spins, me * patches, patches)
    group = jnp.arange(columns, dtype=jnp.int32)[:, None]
    arrival = (jnp.bitwise_xor(group, me) * per_peer + rank).reshape(-1)
    slot = (patch_zone - me * row_count) * capacity + patch_position
    mine = column.reshape(-1) == me
    places = jnp.arange(columns * per_peer, dtype=jnp.int32)
    matched = (arrival[None, :] == places[:, None]) & mine[None, :]
    target = jnp.sum(jnp.where(matched, slot[None, :] + 1, 0), axis=1) - 1

    per_step = capacity // 3
    out_shape = jax.ShapeDtypeStruct(
        (steps * row_count, 1, capacity, side, side), jnp.float32
    )
    regional = None
    for k in range(CHUNKS):
        packed = pl.pallas_call(
            functools.partial(pack_kernel, k * rows, rows),
            out_shape=[jax.ShapeDtypeStruct((per_peer, steps, rows, side), jnp.float32)]
            * columns,
            in_specs=[SMEM, SMEM, SMEM, VMEM],
            out_specs=[VMEM] * columns,
            name=f"pack{k}",
        )(peers, my_rank, turns, ocean_heat_field)
        arrived = [packed[0]] + [
            lax.ppermute(packed[d], "gx", [(i, i ^ d) for i in range(columns)])
            for d in range(1, columns)
        ]
        picked = pl.pallas_call(
            pick_kernel,
            out_shape=jax.ShapeDtypeStruct(
                (row_count * capacity, steps, rows, side), jnp.float32
            ),
            in_specs=[SMEM] + [VMEM] * columns,
            out_specs=VMEM,
            name="pick",
        )(target, *arrived)
        timed = lax.all_to_all(picked, "gy", split_axis=0, concat_axis=0, tiled=True)
        timed = timed.reshape(row_count, capacity, steps, rows, side)
        operands = (zone_patch_tally, timed) + (() if k == 0 else (regional,))
        regional = pl.pallas_call(
            center_kernel,
            grid=(capacity // per_step,),
            out_shape=out_shape,
            in_specs=[
                SMEM,
                pl.BlockSpec((row_count, per_step, steps, rows, side), lambda i: (0, i, 0, 0, 0)),
            ]
            + ([] if k == 0 else [pl.BlockSpec(memory_space=pl.ANY)]),
            out_specs=pl.BlockSpec(
                (steps * row_count, 1, per_step, rows, side),
                functools.partial(lambda k, i: (0, 0, i, k, 0), k),
            ),
            input_output_aliases={} if k == 0 else {2: 0},
            name=f"center{k}",
        )(*operands)
    return regional


def solution(mesh):
    placed = (P("gy", "gx", None, None), P(), P(), P(), P(("gx", "gy")))
    return jax.shard_map(
        on_device,
        mesh=mesh,
        in_specs=placed,
        out_specs=P(None, ("gx", "gy"), None, None, None),
        check_vma=False,
    )
```

```python
import functools

import jax
import jax.numpy as jnp
from jax import lax
from jax.experimental import pallas as pl
from jax.experimental.pallas import tpu as pltpu
from jax.sharding import PartitionSpec as P

CUTS = (0, 1, 2, 3, 4)


SMEM = pl.BlockSpec(memory_space=pltpu.SMEM)
VMEM = pl.BlockSpec(memory_space=pltpu.VMEM)


def mirror(x):
    lane = lax.broadcasted_iota(jnp.int32, x.shape, 1)
    return jnp.take_along_axis(x, x.shape[1] - 1 - lane, axis=1, mode="promise_in_bounds")


def flush(scratch, out_refs, sems, pieces):
    copies = [
        pltpu.make_async_copy(scratch.at[piece], out_ref, sems.at[i])
        for i, (piece, out_ref) in enumerate(zip(pieces, out_refs))
    ]
    for copy in copies:
        copy.start()
    for copy in copies:
        copy.wait()


def pack_kernel(spans, per_peer, places, turns, x_ref, *refs):
    out_refs, scratch, sems = refs[:-2], refs[-2], refs[-1]
    steps, blocks, side, _ = x_ref.shape
    first, last = spans[0][0], spans[-1][1]
    peers = len(out_refs) // len(spans)

    def one(j, carry):
        place = places[j]
        turn = turns[j]

        @pl.when(turn == 0)
        def _():
            for t in range(steps):
                scratch[place, t] = x_ref[t, j, first:last]

        @pl.when(turn == 1)
        def _():
            for t in range(steps):
                scratch[place, t] = mirror(x_ref[t, j]).T[first:last]

        @pl.when(turn == 2)
        def _():
            for t in range(steps):
                scratch[place, t] = mirror(mirror(x_ref[t, j]).T).T[first:last]

        @pl.when(turn == 3)
        def _():
            for t in range(steps):
                scratch[place, t] = mirror(x_ref[t, j].T[first:last])

        return carry

    lax.fori_loop(0, blocks, one, 0)
    pieces = [
        (pl.ds(d * per_peer, per_peer), slice(None), pl.ds(lo - first, hi - lo))
        for lo, hi in spans
        for d in range(peers)
    ]
    flush(scratch, out_refs, sems, pieces)


def pick_kernel(arrivals, target, *refs):
    arrived_refs, out_refs = refs[:arrivals], refs[arrivals:-2]
    scratch, sems = refs[-2], refs[-1]
    per_peer = arrived_refs[0].shape[0]
    capacity = out_refs[0].shape[0]
    for d, arrived_ref in enumerate(arrived_refs):
        for i in range(per_peer):
            to = target[d * per_peer + i]

            @pl.when(to >= 0)
            def _():
                scratch[to] = arrived_ref[i]

    pieces = [(pl.ds(d * capacity, capacity),) for d in range(len(out_refs))]
    flush(scratch, out_refs, sems, pieces)


def center_kernel(groups, tally, origin, *refs):
    z_refs, out_ref = refs[:groups], refs[-1]
    slots, steps, rows, side = z_refs[0].shape
    total = groups * steps
    first_slot = pl.program_id(0) * slots
    for s in range(slots):
        used = first_slot + s < tally[0]

        @pl.when(used)
        def _():
            mean = z_refs[0][s, 0]
            for d in range(groups):
                for t in range(steps):
                    if d + t:
                        mean = mean + z_refs[d][s, t]
            mean = mean * (1.0 / total)
            for d in range(groups):
                for t in range(steps):
                    out_ref[origin[d] * steps + t, 0, s] = z_refs[d][s, t] - mean

        @pl.when(jnp.logical_not(used))
        def _():
            out_ref[:, 0, s] = jnp.zeros((total, rows, side), jnp.float32)


def on_device(ocean_heat_field, patch_zone, patch_position, quarter_spins, zone_patch_tally):
    steps, patches, side, _ = ocean_heat_field.shape
    columns = lax.axis_size("gx")
    row_count = lax.axis_size("gy")
    per_peer = 2 * patches // columns
    capacity = 2 * patches // row_count
    me = lax.axis_index("gx")

    column = (patch_zone // row_count).reshape(columns, patches)
    same = column[:, :, None] == column[:, None, :]
    earlier = jnp.arange(patches)[None, None, :] < jnp.arange(patches)[None, :, None]
    rank = jnp.sum((same & earlier).astype(jnp.int32), axis=2)
    my_column = lax.dynamic_index_in_dim(column, me, 0, keepdims=False)
    my_rank = lax.dynamic_index_in_dim(rank, me, 0, keepdims=False)
    send_places = jnp.bitwise_xor(my_column, me) * per_peer + my_rank
    turns = lax.dynamic_slice_in_dim(quarter_spins, me * patches, patches)
    group = jnp.arange(columns, dtype=jnp.int32)[:, None]
    arrival = (jnp.bitwise_xor(group, me) * per_peer + rank).reshape(-1)
    my_row = lax.axis_index("gy")
    row = jnp.bitwise_xor(patch_zone - me * row_count, my_row)
    slot = row * capacity + patch_position
    origin = jnp.bitwise_xor(jnp.arange(row_count, dtype=jnp.int32), my_row)
    mine = column.reshape(-1) == me
    places = jnp.arange(columns * per_peer, dtype=jnp.int32)
    matched = (arrival[None, :] == places[:, None]) & mine[None, :]
    target = jnp.sum(jnp.where(matched, slot[None, :] + 1, 0), axis=1) - 1

    per_step = capacity // 3
    out_shape = jax.ShapeDtypeStruct(
        (steps * row_count, 1, capacity, side, side), jnp.float32
    )
    hbm = pl.BlockSpec(memory_space=pl.ANY)
    cuts = [side * c // CUTS[-1] for c in CUTS]
    spans = list(zip(cuts[:-1], cuts[1:]))

    def swap(pieces, axis):
        count = len(pieces)
        return pieces[:1] + [
            lax.ppermute(pieces[d], axis, [(i, i ^ d) for i in range(count)])
            for d in range(1, count)
        ]

    def pack(parts, name):
        rows = parts[-1][1] - parts[0][0]
        shapes = [
            jax.ShapeDtypeStruct((per_peer, steps, hi - lo, side), jnp.float32)
            for lo, hi in parts
            for _ in range(columns)
        ]
        flat = pl.pallas_call(
            functools.partial(pack_kernel, parts, per_peer),
            out_shape=shapes,
            in_specs=[SMEM, SMEM, VMEM],
            out_specs=[hbm] * len(shapes),
            scratch_shapes=[
                pltpu.VMEM((columns * per_peer, steps, rows, side), jnp.float32),
                pltpu.SemaphoreType.DMA((len(shapes),)),
            ],
            name=name,
        )(send_places, turns, ocean_heat_field)
        return [list(flat[k * columns : (k + 1) * columns]) for k in range(len(parts))]

    packed = pack(spans[:1], "pack_first") + pack(spans[1:], "pack_rest")
    regional = None
    received = []
    for k in range(len(spans)):
        if k >= 2:
            packed[k], received[k - 2] = lax.optimization_barrier((packed[k], received[k - 2]))
        received.append(swap(packed[k], "gx"))
    for k, (lo, hi) in enumerate(spans):
        rows = hi - lo
        arrived = received[k]
        picked = pl.pallas_call(
            functools.partial(pick_kernel, columns),
            out_shape=[jax.ShapeDtypeStruct((capacity, steps, rows, side), jnp.float32)]
            * row_count,
            in_specs=[SMEM] + [VMEM] * columns,
            out_specs=[hbm] * row_count,
            scratch_shapes=[
                pltpu.VMEM((row_count * capacity, steps, rows, side), jnp.float32),
                pltpu.SemaphoreType.DMA((row_count,)),
            ],
            name=f"pick{k}",
        )(target, *arrived)
        timed = swap(list(picked), "gy")
        earlier_rows = () if k == 0 else (regional,)
        regional = pl.pallas_call(
            functools.partial(center_kernel, row_count),
            grid=(capacity // per_step,),
            out_shape=out_shape,
            in_specs=[SMEM, SMEM]
            + [pl.BlockSpec((per_step, steps, rows, side), lambda i: (i, 0, 0, 0))] * row_count
            + [hbm] * len(earlier_rows),
            out_specs=pl.BlockSpec(
                (steps * row_count, 1, per_step, rows, side),
                functools.partial(lambda at, i: (0, 0, i, at, 0), lo // rows),
            ),
            input_output_aliases={} if k == 0 else {2 + row_count: 0},
            name=f"center{k}",
        )(zone_patch_tally, origin, *timed, *earlier_rows)
    return regional


def solution(mesh):
    placed = (P("gy", "gx", None, None), P(), P(), P(), P(("gx", "gy")))
    return jax.shard_map(
        on_device,
        mesh=mesh,
        in_specs=placed,
        out_specs=P(None, ("gx", "gy"), None, None, None),
        check_vma=False,
    )
```

```python
import functools

import jax
import jax.numpy as jnp
from jax import lax
from jax.experimental import pallas as pl
from jax.experimental.pallas import tpu as pltpu
from jax.sharding import PartitionSpec as P

CUTS = (0, 1, 2, 3, 4)


SMEM = pl.BlockSpec(memory_space=pltpu.SMEM)
VMEM = pl.BlockSpec(memory_space=pltpu.VMEM)


def mirror(x):
    lane = lax.broadcasted_iota(jnp.int32, x.shape, 1)
    return jnp.take_along_axis(x, x.shape[1] - 1 - lane, axis=1, mode="promise_in_bounds")


def flush(scratch, out_refs, sems, pieces):
    copies = [
        pltpu.make_async_copy(scratch.at[piece], out_ref, sems.at[i])
        for i, (piece, out_ref) in enumerate(zip(pieces, out_refs))
    ]
    for copy in copies:
        copy.start()
    for copy in copies:
        copy.wait()


def pack_kernel(spans, per_peer, places, turns, x_ref, *refs):
    out_refs, scratch, sems = refs[:-2], refs[-2], refs[-1]
    steps, blocks, _, _ = x_ref.shape
    first, last = spans[0][0], spans[-1][1]
    peers = len(out_refs) // len(spans)

    def one(j, carry):
        place = places[j]
        turn = turns[j]

        @pl.when(turn == 0)
        def _():
            for t in range(steps):
                scratch[place, t] = x_ref[t, j, first:last]

        @pl.when(turn == 1)
        def _():
            for t in range(steps):
                scratch[place, t] = mirror(x_ref[t, j]).T[first:last]

        @pl.when(turn == 2)
        def _():
            for t in range(steps):
                scratch[place, t] = mirror(mirror(x_ref[t, j]).T).T[first:last]

        @pl.when(turn == 3)
        def _():
            for t in range(steps):
                scratch[place, t] = mirror(x_ref[t, j].T[first:last])

        return carry

    lax.fori_loop(0, blocks, one, 0)
    pieces = [
        (pl.ds(d * per_peer, per_peer), slice(None), pl.ds(lo - first, hi - lo))
        for lo, hi in spans
        for d in range(peers)
    ]
    flush(scratch, out_refs, sems, pieces)


def pick_kernel(arrivals, target, *refs):
    arrived_refs, out_refs = refs[:arrivals], refs[arrivals:-2]
    scratch, sems = refs[-2], refs[-1]
    per_peer = arrived_refs[0].shape[0]
    capacity = out_refs[0].shape[0]
    for d, arrived_ref in enumerate(arrived_refs):
        for i in range(per_peer):
            to = target[d * per_peer + i]

            @pl.when(to >= 0)
            def _():
                scratch[to] = arrived_ref[i]

    pieces = [(pl.ds(d * capacity, capacity),) for d in range(len(out_refs))]
    flush(scratch, out_refs, sems, pieces)


def center_kernel(groups, tally, origin, *refs):
    z_refs, out_ref = refs[:groups], refs[-1]
    slots, steps, rows, side = z_refs[0].shape
    total = groups * steps
    first_slot = pl.program_id(0) * slots
    for s in range(slots):
        used = first_slot + s < tally[0]

        @pl.when(used)
        def _():
            mean = z_refs[0][s, 0]
            for d in range(groups):
                for t in range(steps):
                    if d + t:
                        mean = mean + z_refs[d][s, t]
            mean = mean * (1.0 / total)
            for d in range(groups):
                for t in range(steps):
                    out_ref[origin[d] * steps + t, 0, s] = z_refs[d][s, t] - mean

        @pl.when(jnp.logical_not(used))
        def _():
            out_ref[:, 0, s] = jnp.zeros((total, rows, side), jnp.float32)


def on_device(ocean_heat_field, patch_zone, patch_position, quarter_spins, zone_patch_tally):
    steps, patches, side, _ = ocean_heat_field.shape
    columns = lax.axis_size("gx")
    row_count = lax.axis_size("gy")
    per_peer = 2 * patches // columns
    capacity = 2 * patches // row_count
    me = lax.axis_index("gx")

    column = (patch_zone // row_count).reshape(columns, patches)
    same = column[:, :, None] == column[:, None, :]
    earlier = jnp.arange(patches)[None, None, :] < jnp.arange(patches)[None, :, None]
    rank = jnp.sum((same & earlier).astype(jnp.int32), axis=2)
    my_column = lax.dynamic_index_in_dim(column, me, 0, keepdims=False)
    my_rank = lax.dynamic_index_in_dim(rank, me, 0, keepdims=False)
    send_places = jnp.bitwise_xor(my_column, me) * per_peer + my_rank
    turns = lax.dynamic_slice_in_dim(quarter_spins, me * patches, patches)
    group = jnp.arange(columns, dtype=jnp.int32)[:, None]
    arrival = (jnp.bitwise_xor(group, me) * per_peer + rank).reshape(-1)
    my_row = lax.axis_index("gy")
    row = jnp.bitwise_xor(patch_zone - me * row_count, my_row)
    slot = row * capacity + patch_position
    origin = jnp.bitwise_xor(jnp.arange(row_count, dtype=jnp.int32), my_row)
    mine = column.reshape(-1) == me
    places = jnp.arange(columns * per_peer, dtype=jnp.int32)
    matched = (arrival[None, :] == places[:, None]) & mine[None, :]
    target = jnp.sum(jnp.where(matched, slot[None, :] + 1, 0), axis=1) - 1

    per_step = capacity // 3
    out_shape = jax.ShapeDtypeStruct(
        (steps * row_count, 1, capacity, side, side), jnp.float32
    )
    hbm = pl.BlockSpec(memory_space=pl.ANY)
    cuts = [side * c // CUTS[-1] for c in CUTS]
    spans = list(zip(cuts[:-1], cuts[1:]))

    def swap(pieces, axis):
        count = len(pieces)
        moved = []
        for d in range(1, count):
            moved.append(lax.ppermute(pieces[d], axis, [(i, i ^ d) for i in range(count)]))
        return pieces[:1] + moved

    def pack(parts):
        rows = parts[-1][1] - parts[0][0]
        shapes = [
            jax.ShapeDtypeStruct((per_peer, steps, hi - lo, side), jnp.float32)
            for lo, hi in parts
            for _ in range(columns)
        ]
        flat = pl.pallas_call(
            functools.partial(pack_kernel, parts, per_peer),
            out_shape=shapes,
            in_specs=[SMEM, SMEM, VMEM],
            out_specs=[hbm] * len(shapes),
            scratch_shapes=[
                pltpu.VMEM((columns * per_peer, steps, rows, side), jnp.float32),
                pltpu.SemaphoreType.DMA((len(shapes),)),
            ],
        )(send_places, turns, ocean_heat_field)
        return [list(flat[k * columns : (k + 1) * columns]) for k in range(len(parts))]

    def center(k, timed, regional):
        lo, hi = spans[k]
        rows = hi - lo
        earlier_rows = () if k == 0 else (regional,)
        return pl.pallas_call(
            functools.partial(center_kernel, row_count),
            grid=(capacity // per_step,),
            out_shape=out_shape,
            in_specs=[SMEM, SMEM]
            + [pl.BlockSpec((per_step, steps, rows, side), lambda i: (i, 0, 0, 0))] * row_count
            + [hbm] * len(earlier_rows),
            out_specs=pl.BlockSpec(
                (steps * row_count, 1, per_step, rows, side),
                functools.partial(lambda at, i: (0, 0, i, at, 0), lo // rows),
            ),
            input_output_aliases={} if k == 0 else {2 + row_count: 0},
        )(zone_patch_tally, origin, *timed, *earlier_rows)

    packed = pack(spans[:1]) + pack(spans[1:])
    regional = None
    picked = None
    for k, (lo, hi) in enumerate(spans):
        rows = hi - lo
        if k >= 1:
            packed[k], picked = lax.optimization_barrier((packed[k], picked))
            timed = swap(picked, "gy")
            regional = center(k - 1, timed, regional)
        arrived = swap(packed[k], "gx")
        picked = pl.pallas_call(
            functools.partial(pick_kernel, columns),
            out_shape=[jax.ShapeDtypeStruct((capacity, steps, rows, side), jnp.float32)]
            * row_count,
            in_specs=[SMEM] + [VMEM] * columns,
            out_specs=[hbm] * row_count,
            scratch_shapes=[
                pltpu.VMEM((row_count * capacity, steps, rows, side), jnp.float32),
                pltpu.SemaphoreType.DMA((row_count,)),
            ],
        )(target, *arrived)
        picked = list(picked)
    regional = center(len(spans) - 1, swap(picked, "gy"), regional)
    return regional


def solution(mesh):
    placed = (P("gy", "gx", None, None), P(), P(), P(), P(("gx", "gy")))
    return jax.shard_map(
        on_device,
        mesh=mesh,
        in_specs=placed,
        out_specs=P(None, ("gx", "gy"), None, None, None),
        check_vma=False,
    )
```
